128 devices in a mesh: row: 8 (over x_hi, z), col: 16 (over x_lo, y, core).
Axes of the slice: x: 4 (x_hi: 2, x_lo: 2; x = x_hi * 2 + x_lo), y: 4, z: 4, core: 2. Of those that a mesh axis runs over, the one named last changes fastest.
Arguments:
- features: bfloat16 [384, 256, 512], P('row', 'col'), may hold values from -12 to 12
- cotangent: bfloat16 [384, 256, 512], P('row', 'col'), may hold values from -6 to 6
- w_query: bfloat16 [512, 512], replicated, may hold values from -0.53033009 to 0.53033009
- w_key: bfloat16 [512, 512], replicated, may hold values from -0.53033009 to 0.53033009
- w_value: bfloat16 [512, 512], replicated, may hold values from -0.25 to 0.25
- w_out: bfloat16 [512, 512], replicated, may hold values from -0.25 to 0.25
Outputs:
- layer_out: bfloat16 [384, 256, 512], P('row', 'col')
- grad_features: bfloat16 [384, 256, 512], P('row', 'col')
- grad_query: float32 [512, 512], replicated
- grad_key: float32 [512, 512], replicated
- grad_value: float32 [512, 512], replicated
- grad_proj: float32 [512, 512], replicated
The draws below stay inside these ranges and needn't reach their ends.
All inputs are finite; a program needn't handle non-finite values.
Results may differ from the reference program's by a relative error of at most 0.012.
The reference program's roundings to bfloat16 on the way count: a program that leaves them out, or rounds other values in their place, can miss the bound.
Values may be sent and summed in bfloat16 or wider, within the bound.
A program may use at most 128 MiB of HBM per device.

```python
import math
import jax
import jax.numpy as jnp
from jax import lax

C = 512
HEADS = 8
H = 384
W = 256


def block_field(key):
    coarse = jax.random.normal(jax.random.fold_in(key, 7), (H // 8, W // 8, C), jnp.float32)
    coarse = 1.5 * coarse
    return jnp.repeat(jnp.repeat(coarse, 8, axis=0), 8, axis=1)


def draw_features(key, part):
    normal_part = jax.random.normal(jax.random.fold_in(key, 3), (H, W, C), jnp.float32)
    common = block_field(key)
    return jnp.clip(common + normal_part, -8.0, 8.0).astype(jnp.bfloat16)


def paired_weight(key, salt):
    private = jax.random.normal(jax.random.fold_in(key, salt), (C, C), jnp.float32)
    limit = 12.0 / math.sqrt(C)
    mixed = private / math.sqrt(C)
    return jnp.clip(mixed, -limit, limit).astype(jnp.bfloat16)


def draw_w_query(key, part):
    return paired_weight(key, 211)


def draw_w_key(key, part):
    return paired_weight(key, 307)


def level_of(own_key, shape, cuts, low, top_value):
    def one(axis_at, blocks):
        heights = jax.random.uniform(jax.random.fold_in(jax.random.fold_in(own_key, 6), axis_at), (blocks,), jnp.float32, low / len(cuts), top_value / len(cuts))
        return jnp.repeat(jnp.exp(heights), shape[axis_at] // blocks).reshape((-1,) + (1,) * (len(shape) - axis_at - 1))

    level = one(*cuts[0])
    for cut in cuts[1:]:
        level = level * one(*cut)
    return level


def normal_values(own_key, shape, spread, reach, split=(), held_as=jnp.bfloat16):
    loudness = level_of(own_key, shape, split, -0.22, 0.18) if split else 1.0
    drawn = jax.random.normal(own_key, shape, jnp.float32) * spread * loudness
    return jnp.minimum(jnp.maximum(drawn, -reach), reach).astype(held_as)


def setup_inputs(seed: int = 0) -> dict:
    splits = jax.random.split(jax.random.key(seed), 7)
    return {
        "features": draw_features(jax.random.fold_in(splits[6], 71), 0),
        "cotangent": normal_values(splits[1], (H, W, C), 1.0, 6.0, ((0, 8), (1, 16))),
        "w_query": draw_w_query(jax.random.fold_in(splits[6], 71), 0),
        "w_key": draw_w_key(jax.random.fold_in(splits[6], 71), 0),
        "w_value": normal_values(splits[4], (C, C), C ** -0.5, 0.25),
        "w_out": normal_values(splits[5], (C, C), C ** -0.5, 0.25),
    }


NEG_FILL = -1e30


def product_of(form, left, right):
    return jnp.einsum(form, left.astype(jnp.float32), right.astype(jnp.float32))


def project(left, weight):
    return jnp.dot(left, weight, preferred_element_type=jnp.float32).astype(jnp.bfloat16)


def times_transposed(left, weight):
    return lax.dot_general(left, weight, (((1,), (1,)), ((), ())), preferred_element_type=jnp.float32)


def inner_sum(left, right):
    return lax.dot_general(left, right, (((0,), (0,)), ((), ())), preferred_element_type=jnp.float32)


def inner_exact(left, right):
    return lax.dot_general(left, right, (((0,), (0,)), ((), ())), precision=lax.Precision.HIGHEST, preferred_element_type=jnp.float32)


def transposed_exact(left, weight):
    return lax.dot_general(left, weight.astype(jnp.float32), (((1,), (1,)), ((), ())), precision=lax.Precision.HIGHEST, preferred_element_type=jnp.float32)


def to_windows(field):
    tile_rows, tile_cols, feature = field.shape
    blocks = field.reshape(tile_rows // 16, 16, tile_cols // 16, 16, feature)
    return blocks.transpose(0, 2, 1, 3, 4).reshape(-1, 256, feature)


def from_windows(blocks, tile_rows, tile_cols):
    feature = blocks.shape[-1]
    field = blocks.reshape(tile_rows // 16, tile_cols // 16, 16, 16, feature)
    return field.transpose(0, 2, 1, 3, 4).reshape(tile_rows, tile_cols, feature)


def split_heads(field, heads):
    blocks = to_windows(field)
    count, per_window, feature = blocks.shape
    return blocks.reshape(count, per_window, heads, feature // heads).transpose(2, 0, 1, 3)


def join_heads(stacked, tile_rows, tile_cols):
    heads, count, per_window, depth = stacked.shape
    blocks = stacked.transpose(1, 2, 0, 3).reshape(count, per_window, heads * depth)
    return from_windows(blocks, tile_rows, tile_cols)


def summary_heads(table, heads):
    count, feature = table.shape
    return table.reshape(count, heads, feature // heads).transpose(1, 0, 2)


def join_summary(stacked):
    heads, count, depth = stacked.shape
    return stacked.transpose(1, 0, 2).reshape(count, heads * depth)


def region_allowed(row_flag, col_flag):
    region = row_flag.astype(jnp.int32)[:, None] * 2 + col_flag.astype(jnp.int32)[None, :]
    blocks = to_windows(region[:, :, None])[:, :, 0]
    return blocks[:, :, None] == blocks[:, None, :]


def pool_field(field):
    tile_rows, tile_cols, feature = field.shape
    blocks = field.astype(jnp.float32).reshape(tile_rows // 8, 8, tile_cols // 8, 8, feature)
    return jnp.mean(blocks, axis=(1, 3)).reshape(-1, feature).astype(jnp.bfloat16)


def spread_pool(grad_pooled, tile_rows, tile_cols):
    feature = grad_pooled.shape[-1]
    blocks = grad_pooled.reshape(tile_rows // 8, 1, tile_cols // 8, 1, feature) / 64.0
    blocks = jnp.broadcast_to(blocks, (tile_rows // 8, 8, tile_cols // 8, 8, feature))
    return blocks.reshape(tile_rows, tile_cols, feature)


def one_head(operands, allowed, scale):
    queries, keys_win, values_win, summary_keys, summary_values, grad_attn = operands
    scores_win = jnp.where(allowed, product_of("wid,wjd->wij", queries, keys_win) * scale, NEG_FILL)
    scores_sum = product_of("wid,md->wim", queries, summary_keys) * scale
    highest = jnp.maximum(jnp.max(scores_win, axis=-1), jnp.max(scores_sum, axis=-1))[..., None]
    expo_win = jnp.exp(scores_win - highest)
    expo_sum = jnp.exp(scores_sum - highest)
    denominator = jnp.sum(expo_win, axis=-1, keepdims=True) + jnp.sum(expo_sum, axis=-1, keepdims=True)
    probs_win = expo_win / denominator
    probs_sum = expo_sum / denominator
    weights_win = probs_win.astype(jnp.bfloat16)
    weights_sum = probs_sum.astype(jnp.bfloat16)
    attended = product_of("wij,wjd->wid", weights_win, values_win) + product_of("wim,md->wid", weights_sum, summary_values)
    dprob_win = product_of("wid,wjd->wij", grad_attn, values_win)
    dprob_sum = product_of("wid,md->wim", grad_attn, summary_values)
    inner = jnp.sum(probs_win * dprob_win, axis=-1, keepdims=True) + jnp.sum(probs_sum * dprob_sum, axis=-1, keepdims=True)
    dscore_win = (probs_win * (dprob_win - inner) * scale).astype(jnp.bfloat16)
    dscore_sum = (probs_sum * (dprob_sum - inner) * scale).astype(jnp.bfloat16)
    grad_q = product_of("wij,wjd->wid", dscore_win, keys_win) + product_of("wim,md->wid", dscore_sum, summary_keys)
    grad_k = product_of("wij,wid->wjd", dscore_win, queries)
    grad_v = product_of("wij,wid->wjd", weights_win, grad_attn)
    grad_sk = product_of("wim,wid->md", dscore_sum, queries)
    grad_sv = product_of("wim,wid->md", weights_sum, grad_attn)
    return (attended.astype(jnp.bfloat16), grad_q.astype(jnp.bfloat16), grad_k.astype(jnp.bfloat16),
            grad_v.astype(jnp.bfloat16), grad_sk, grad_sv)


def attend(queries, keys, values, summary_keys, summary_values, grad_attn, allowed, heads):
    tile_rows, tile_cols, feature = queries.shape
    scale = float(feature // heads) ** -0.5
    operands = (split_heads(queries, heads), split_heads(keys, heads), split_heads(values, heads),
                summary_heads(summary_keys, heads), summary_heads(summary_values, heads), split_heads(grad_attn, heads))
    results = lax.map(lambda stacked: one_head(stacked, allowed, scale), operands)
    attended, grad_q, grad_k, grad_v, grad_sk, grad_sv = results
    return (join_heads(attended, tile_rows, tile_cols), join_heads(grad_q, tile_rows, tile_cols),
            join_heads(grad_k, tile_rows, tile_cols), join_heads(grad_v, tile_rows, tile_cols),
            join_summary(grad_sk), join_summary(grad_sv))


def reference(features, cotangent, w_query, w_key, w_value, w_out):
    shifted = jnp.roll(features, (8, 8), axis=(0, 1))
    tile_rows, tile_cols, feature = shifted.shape
    flat = shifted.reshape(-1, feature)
    queries = project(flat, w_query).reshape(shifted.shape)
    keys = project(flat, w_key).reshape(shifted.shape)
    values = project(flat, w_value).reshape(shifted.shape)
    pooled = pool_field(shifted)
    summary_keys = project(pooled, w_key)
    summary_values = project(pooled, w_value)
    grad_flat = cotangent.reshape(-1, feature)
    grad_attn = times_transposed(grad_flat, w_out).astype(jnp.bfloat16).reshape(shifted.shape)
    allowed = region_allowed(jnp.arange(tile_rows) < 8, jnp.arange(tile_cols) < 8)
    attended, grad_q, grad_k, grad_v, grad_sk, grad_sv = attend(queries, keys, values, summary_keys, summary_values, grad_attn, allowed, HEADS)
    attended_flat = attended.reshape(-1, feature)
    layer_out = (flat.astype(jnp.float32) + jnp.dot(attended_flat, w_out, preferred_element_type=jnp.float32)).astype(jnp.bfloat16).reshape(shifted.shape)
    grad_q = grad_q.reshape(-1, feature)
    grad_k = grad_k.reshape(-1, feature)
    grad_v = grad_v.reshape(-1, feature)
    grad_pooled = transposed_exact(grad_sk, w_key) + transposed_exact(grad_sv, w_value)
    local_part = times_transposed(grad_q, w_query) + times_transposed(grad_k, w_key) + times_transposed(grad_v, w_value)
    grad_field = cotangent.astype(jnp.float32) + local_part.reshape(shifted.shape) + spread_pool(grad_pooled, tile_rows, tile_cols)
    pooled_wide = pooled.astype(jnp.float32)
    grad_query = inner_sum(flat, grad_q)
    grad_key = inner_sum(flat, grad_k) + inner_exact(pooled_wide, grad_sk)
    grad_value = inner_sum(flat, grad_v) + inner_exact(pooled_wide, grad_sv)
    grad_proj = inner_sum(attended_flat, grad_flat)
    return layer_out, grad_field.astype(jnp.bfloat16), grad_query, grad_key, grad_value, grad_proj
```

```python
import jax, jax.numpy as jnp
from jax import lax
from jax.experimental import pallas as pl
from jax.experimental.pallas import tpu as pltpu
from jax.sharding import PartitionSpec as P

C = 512
NS = 1536
NT = 768
F32, BF16 = jnp.float32, jnp.bfloat16


def dot(a, b):
    return jnp.dot(a, b, preferred_element_type=F32)


def dot_t(a, b):
    return lax.dot_general(a, b, (((1,), (1,)), ((), ())), preferred_element_type=F32)


def main_kernel(x_ref, cot_ref, pool_ref, wq_ref, wk_ref, wv_ref, wo_ref,
                out_ref, base_ref, gp_ref, wg_ref,
                kp, vp, kt, vt, qt, gt, s_scr, we, ds, att_t, gq_t, gk, gv, acc_k, acc_v):
    first_row = lax.axis_index("row") == 0
    first_col = lax.axis_index("col") == 0
    def put_keys(src, first, count):
        for w_ref, dst, dst_t in ((wk_ref, kp, kt), (wv_ref, vp, vt)):
            val = src(w_ref).astype(BF16)
            for p in range(4):
                dst[p, first:first + count, :] = val[:, p * 128:(p + 1) * 128]
            for i in range(count // 256):
                tr = val[i * 256:(i + 1) * 256].T
                for h in range(8):
                    dst_t[h, 0:64, first + i * 256:first + (i + 1) * 256] = tr[h * 64:(h + 1) * 64]
    for i in range(3):
        put_keys(lambda w: dot(pool_ref[0, i * 512:(i + 1) * 512], w[0:256]) + dot(pool_ref[1, i * 512:(i + 1) * 512], w[256:512]),
                 i * 512, 512)
    for w in range(3):
        xw = x_ref[w * 256:(w + 1) * 256]
        put_keys(lambda wr: dot(xw, wr[...]), NS + w * 256, 256)
        qt[w] = (dot(xw, wq_ref[...]).astype(BF16) * jnp.asarray(0.125, BF16)).T
        gt[w] = dot_t(wo_ref[...], cot_ref[w * 256:(w + 1) * 256]).astype(BF16)
    tail = (lax.broadcasted_iota(jnp.int32, (16, 2304), 0) == 0).astype(F32).astype(BF16)
    for h in range(8):
        vt[h, 64:80, :] = tail
    acc_k[...] = jnp.zeros_like(acc_k)
    acc_v[...] = jnp.zeros_like(acc_v)

    def step(it, carry):
        p = it // 3
        w = it % 3
        kwin = pl.ds(pl.multiple_of(NS + w * 256, 256), 256)
        def regions(axis):
            idx = lax.broadcasted_iota(jnp.int32, (256, 256), axis)
            r = jnp.where(((idx // 16) < 8) & first_row & (w == 0), 2, 0)
            return r + jnp.where(((idx % 16) < 8) & first_col, 1, 0)
        def rows_of(ref, c):
            return ref[p, c * 256:(c + 1) * 256, :] if c < 6 else ref[p, kwin, :]
        zeros = jnp.zeros((64, 256), BF16)
        pads = (lambda v: jnp.concatenate([v, zeros], 0), lambda v: jnp.concatenate([zeros, v], 0))
        sides = []
        for hh in range(2):
            h = p * 2 + hh
            hs = pl.ds(pl.multiple_of(h * 64, 64), 64)
            q = qt[w, hs, :]
            g = gt[w, hs, :]
            qm, gm = pads[hh](q), pads[hh](g)
            m8 = None
            for c in range(7):
                s = dot(rows_of(kp, c), qm)
                if c == 6:
                    s = jnp.where(regions(0) == regions(1), s, -1e30)
                s_scr[hh, c * 256:(c + 1) * 256, :] = s
                top = jnp.max(s.reshape(32, 8, 256), axis=0)
                m8 = top if m8 is None else jnp.maximum(m8, top)
            m = jnp.max(m8, axis=0, keepdims=True)
            for c in range(7):
                we[hh, c * 256:(c + 1) * 256, :] = jnp.exp(s_scr[hh, c * 256:(c + 1) * 256, :] - m).astype(BF16)
            a80 = dot(vt[h, :, 0:NS], we[hh, 0:NS, :]) + dot(vt[h, :, kwin], we[hh, NS:, :])
            rinv = 1.0 / a80[64:65, :]
            att = a80[0:64, :] * rinv
            att_t[w, hs, :] = att.astype(BF16)
            inner = jnp.sum(att * g.astype(F32), axis=0, keepdims=True)
            for c in range(7):
                dp = dot(rows_of(vp, c), gm)
                ds[hh, c * 256:(c + 1) * 256, :] = (we[hh, c * 256:(c + 1) * 256, :].astype(F32) * (dp - inner)).astype(BF16)
            dq = dot(kt[h, :, 0:NS], ds[hh, 0:NS, :]) + dot(kt[h, :, kwin], ds[hh, NS:, :])
            gq_t[w, hs, :] = (dq * (rinv * 0.125)).astype(BF16)
            sides.append(((qm.astype(F32) * rinv).astype(BF16), (gm.astype(F32) * rinv).astype(BF16)))
        for c in range(7):
            rows = slice(c * 256, (c + 1) * 256)
            dk = dot_t(ds[0, rows, :], sides[0][0]) + dot_t(ds[1, rows, :], sides[1][0])
            dv = dot_t(we[0, rows, :], sides[0][1]) + dot_t(we[1, rows, :], sides[1][1])
            if c < 6:
                acc_k[p, rows, :] += dk
                acc_v[p, rows, :] += dv
            else:
                gk[w, p] = dk.astype(BF16)
                gv[w, p] = dv.astype(BF16)
        return carry

    lax.fori_loop(0, 12, step, 0)

    wg_acc = [None] * 4
    for w in range(3):
        rows = slice(w * 256, (w + 1) * 256)
        xw = x_ref[rows]
        cw = cot_ref[rows]
        a_t = att_t[w]
        out_ref[rows] = (xw.astype(F32) + dot(a_t.T, wo_ref[...])).astype(BF16)
        gqw = gq_t[w].T
        gkw = jnp.concatenate([gk[w, p] for p in range(4)], 1)
        gvw = jnp.concatenate([gv[w, p] for p in range(4)], 1)
        base_ref[rows] = cw.astype(F32) + dot_t(gqw, wq_ref[...]) + dot_t(gkw, wk_ref[...]) + dot_t(gvw, wv_ref[...])
        xt = xw.T
        for i, (a, b) in enumerate(((xt, gqw), (xt, gkw), (xt, gvw), (a_t, cw))):
            t = dot(a, b)
            wg_acc[i] = t if w == 0 else wg_acc[i] + t
    sk = jnp.concatenate([acc_k[p].astype(BF16) for p in range(4)], 1)
    sv = jnp.concatenate([acc_v[p].astype(BF16) for p in range(4)], 1)
    for i in range(3):
        rows = slice(i * 512, (i + 1) * 512)
        gp_ref[rows] = (dot_t(sk[rows], wk_ref[...]) + dot_t(sv[rows], wv_ref[...])).astype(BF16)
        pt = jnp.concatenate([pool_ref[0, rows].T, pool_ref[1, rows].T], 0)
        wg_acc[1] += dot(pt, sk[rows])
        wg_acc[2] += dot(pt, sv[rows])
    for i in range(4):
        wg_ref[i * 512:(i + 1) * 512] = wg_acc[i].astype(BF16)


def main_call(x, cot, pool, wq, wk, wv, wo):
    vm = pl.BlockSpec(memory_space=pltpu.VMEM)
    return pl.pallas_call(
        main_kernel,
        out_shape=(jax.ShapeDtypeStruct((NT, C), BF16), jax.ShapeDtypeStruct((NT, C), F32),
                   jax.ShapeDtypeStruct((NS, C), BF16), jax.ShapeDtypeStruct((2048, C), BF16)),
        in_specs=[vm] * 7, out_specs=(vm,) * 4,
        scratch_shapes=[
            pltpu.VMEM((4, 2304, 128), BF16), pltpu.VMEM((4, 2304, 128), BF16),
            pltpu.VMEM((8, 64, 2304), BF16), pltpu.VMEM((8, 80, 2304), BF16),
            pltpu.VMEM((3, 512, 256), BF16), pltpu.VMEM((3, 512, 256), BF16),
            pltpu.VMEM((2, 1792, 256), F32), pltpu.VMEM((2, 1792, 256), BF16), pltpu.VMEM((2, 1792, 256), BF16),
            pltpu.VMEM((3, 512, 256), BF16), pltpu.VMEM((3, 512, 256), BF16),
            pltpu.VMEM((3, 4, 256, 128), BF16), pltpu.VMEM((3, 4, 256, 128), BF16),
            pltpu.VMEM((4, NS, 128), F32), pltpu.VMEM((4, NS, 128), F32),
        ],
        compiler_params=pltpu.CompilerParams(vmem_limit_bytes=60 * 1024 * 1024),
        name="attention",
    )(x, cot, pool, wq, wk, wv, wo)


ROWS, COLS, CHIPS = 8, 16, 64
MESH_ID = pl.DeviceIdType.MESH


def place():
    row, col = lax.axis_index("row"), lax.axis_index("col")
    core = lax.rem(col, 2)
    return row, col, core, row * 8 + lax.div(col, 2)


def chip_device(chip, core):
    return (lax.div(chip, 8), lax.rem(chip, 8) * 2 + core)


def neighbour(row, col, down, right):
    return (lax.rem(row + down + ROWS, ROWS), lax.rem(col + right + COLS, COLS))


def meet(row, col, core, chip):
    barrier = pltpu.get_barrier_semaphore()

    def greet(i, carry):
        pl.semaphore_signal(barrier, inc=1, device_id=chip_device(lax.rem(chip + i, CHIPS), core), device_id_type=MESH_ID)
        return carry

    lax.fori_loop(1, CHIPS, greet, 0)
    for down, right in ((0, 1), (1, 1), (0, -1), (-1, -1)):
        pl.semaphore_signal(barrier, inc=1, device_id=neighbour(row, col, down, right), device_id_type=MESH_ID)
    return barrier


def remote(src, dst, send, recv, device):
    return pltpu.make_async_remote_copy(src_ref=src, dst_ref=dst, send_sem=send, recv_sem=recv,
                                        device_id=device, device_id_type=MESH_ID)


def to_all_chips(src_of, dst, send, recv, chip, core):
    def one(i, carry):
        peer = lax.rem(chip + i, CHIPS)
        remote(src_of(peer), dst, send, recv, chip_device(peer, core)).start()
        return carry

    lax.fori_loop(1, CHIPS, one, 0)


def drain(buf, sem):
    pltpu.make_async_copy(buf, buf, sem).wait()


def gather_kernel(f_ref, shifted_ref, pool_ref, mean, other, mine, sem_s, sem_r):
    row, col, core, chip = place()
    partner = (row, col + 1 - 2 * core)
    barrier = meet(row, col, core, chip)
    for i in range(6):
        total = jnp.sum(f_ref[8 * i:8 * i + 8].astype(F32), axis=0)
        mean[2 * i:2 * i + 2, :] = jnp.sum(total.reshape(2, 8, C), axis=1) * (1.0 / 64.0)
    mean[12:16, :] = jnp.zeros((4, C), F32)
    pl.semaphore_wait(barrier, CHIPS - 1 + 4)
    swap = remote(mean.at[:, pl.ds(pl.multiple_of((1 - core) * 256, 256), 256)], other, sem_s.at[0], sem_r.at[0], partner)
    swap.start()
    halo = [
        remote(f_ref.at[0:40, 8:16], shifted_ref.at[8:48, 0:8], sem_s.at[1], sem_r.at[1], neighbour(row, col, 0, 1)),
        remote(f_ref.at[40:48, 0:8], shifted_ref.at[0:8, 8:16], sem_s.at[2], sem_r.at[2], neighbour(row, col, 1, 0)),
        remote(f_ref.at[40:48, 8:16], shifted_ref.at[0:8, 0:8], sem_s.at[3], sem_r.at[3], neighbour(row, col, 1, 1)),
    ]
    swap.wait()
    own = mean[:, pl.ds(pl.multiple_of(core * 256, 256), 256)]
    got = other[...]
    first = jnp.where(core == 0, own, got)
    second = jnp.where(core == 0, got, own)
    mine[...] = jnp.concatenate([first[0:12], second[0:12]], 0).astype(BF16)
    to_all_chips(lambda peer: mine, pool_ref.at[core, chip], sem_s.at[4], sem_r.at[4], chip, core)
    for copy in halo:
        copy.start()
    keep = pltpu.make_async_copy(mine, pool_ref.at[core, chip], sem_s.at[6])
    keep.start()
    shifted_ref[8:48, 8:16, :] = f_ref[0:40, 0:8, :]
    keep.wait()
    drain(pool_ref.at[core, 0:CHIPS - 1], sem_r.at[4])
    last = remote(pool_ref.at[core], pool_ref.at[core], sem_s.at[5], sem_r.at[5], partner)
    last.start()
    for copy in halo:
        copy.wait()
    drain(pool_ref.at[core, 0:CHIPS - 1], sem_s.at[4])
    last.wait()


def gather_call(features):
    vm = pl.BlockSpec(memory_space=pltpu.VMEM)
    return pl.pallas_call(
        gather_kernel,
        out_shape=(jax.ShapeDtypeStruct((48, 16, C), BF16), jax.ShapeDtypeStruct((2, CHIPS, 24, 256), BF16)),
        in_specs=[vm], out_specs=(vm, vm),
        scratch_shapes=[pltpu.VMEM((16, C), F32), pltpu.VMEM((16, 256), F32), pltpu.VMEM((24, 256), BF16),
                        pltpu.SemaphoreType.DMA((7,)), pltpu.SemaphoreType.DMA((6,))],
        compiler_params=pltpu.CompilerParams(collective_id=0, has_side_effects=True),
        name="gather",
    )(features)


def reduce_kernel(gp_ref, wg_ref, pooled_ref, weights_ref,
                  gp_in, wg_in, gp_s, wg_s, gp_r, wg_r, half, half_in, block, block_in, mine, sem_s, sem_r):
    row, col, core, chip = place()
    partner = (row, col + 1 - 2 * core)
    barrier = meet(row, col, core, chip)
    pl.semaphore_wait(barrier, CHIPS - 1 + 4)
    theirs = pl.ds(pl.multiple_of((1 - core) * 256, 256), 256)
    ours = pl.ds(pl.multiple_of(core * 256, 256), 256)
    swap_w = remote(wg_ref.at[:, :, theirs], wg_in, sem_s.at[0], sem_r.at[0], partner)
    swap_g = remote(gp_ref.at[:, :, theirs], gp_in, sem_s.at[1], sem_r.at[1], partner)
    swap_w.start()
    swap_g.start()

    def add_up(a, b, dst):
        def one(i, carry):
            dst[i] = (a[i, :, ours].astype(F32) + b[i].astype(F32)).astype(BF16)
            return carry
        lax.fori_loop(0, CHIPS, one, 0)

    def total(buf, rows):
        def one(i, carry):
            return carry + buf[i].astype(F32)
        return lax.fori_loop(0, CHIPS, one, jnp.zeros((rows, 256), F32))

    swap_w.wait()
    add_up(wg_ref, wg_in, wg_s)
    to_all_chips(lambda peer: wg_s.at[peer], wg_r.at[chip], sem_s.at[2], sem_r.at[2], chip, core)
    swap_g.wait()
    add_up(gp_ref, gp_in, gp_s)
    to_all_chips(lambda peer: gp_s.at[peer], gp_r.at[chip], sem_s.at[3], sem_r.at[3], chip, core)
    wg_r[chip] = wg_s[chip]
    gp_r[chip] = gp_s[chip]
    drain(wg_r.at[0:CHIPS - 1], sem_r.at[2])
    mine[...] = total(wg_r, 32).astype(BF16)
    to_all_chips(lambda peer: mine, weights_ref.at[core, chip], sem_s.at[4], sem_r.at[4], chip, core)
    keep = pltpu.make_async_copy(mine, weights_ref.at[core, chip], sem_s.at[7])
    keep.start()
    drain(gp_r.at[0:CHIPS - 1], sem_r.at[3])
    half[...] = total(gp_r, 24)
    swap_h = remote(half, half_in, sem_s.at[5], sem_r.at[5], partner)
    swap_h.start()
    swap_h.wait()
    own, got = half[...], half_in[...]
    both = jnp.concatenate([jnp.where(core == 0, own, got), jnp.where(core == 0, got, own)], 1)
    block[0:12, :] = jnp.where(core == 0, both[0:12], both[12:24])
    block[12:16, :] = jnp.zeros((4, C), F32)
    spread = [remote(block, block_in.at[k], sem_s.at[8 + k], sem_r.at[6 + k], neighbour(row, col, *way))
              for k, way in enumerate(((0, 1), (1, 0), (1, 1)))]
    for copy in spread:
        copy.start()
    for copy in spread:
        copy.wait()
    for i in range(6):
        for j in range(2):
            src = (5 if i == 0 else i - 1) * 2 + 1 - j
            if i == 0:
                val = block_in[2, src:src + 1, :] if j == 0 else block_in[1, src:src + 1, :]
            else:
                val = block_in[0, src:src + 1, :] if j == 0 else block[src:src + 1, :]
            pooled_ref[2 * i + j:2 * i + j + 1, :] = val
    keep.wait()
    drain(weights_ref.at[core, 0:CHIPS - 1], sem_r.at[4])
    last = remote(weights_ref.at[core], weights_ref.at[core], sem_s.at[6], sem_r.at[9], partner)
    last.start()
    drain(wg_r.at[0:CHIPS - 1], sem_s.at[2])
    drain(gp_r.at[0:CHIPS - 1], sem_s.at[3])
    drain(weights_ref.at[core, 0:CHIPS - 1], sem_s.at[4])
    last.wait()


def reduce_call(gp, wg):
    vm = pl.BlockSpec(memory_space=pltpu.VMEM)
    return pl.pallas_call(
        reduce_kernel,
        out_shape=(jax.ShapeDtypeStruct((12, C), F32), jax.ShapeDtypeStruct((2, CHIPS, 32, 256), BF16)),
        in_specs=[vm, vm], out_specs=(vm, vm),
        scratch_shapes=[
            pltpu.VMEM((CHIPS, 24, 256), BF16), pltpu.VMEM((CHIPS, 32, 256), BF16),
            pltpu.VMEM((CHIPS, 24, 256), BF16), pltpu.VMEM((CHIPS, 32, 256), BF16),
            pltpu.VMEM((CHIPS, 24, 256), BF16), pltpu.VMEM((CHIPS, 32, 256), BF16),
            pltpu.VMEM((24, 256), F32), pltpu.VMEM((24, 256), F32),
            pltpu.VMEM((16, C), F32), pltpu.VMEM((3, 16, C), F32), pltpu.VMEM((32, 256), BF16),
            pltpu.SemaphoreType.DMA((11,)), pltpu.SemaphoreType.DMA((10,)),
        ],
        compiler_params=pltpu.CompilerParams(collective_id=1, has_side_effects=True),
        name="reduce",
    )(gp.reshape(CHIPS, 24, C), wg.reshape(CHIPS, 32, C))


def body(features, cotangent, w_query, w_key, w_value, w_out):
    shifted, pool = gather_call(features)
    out, base, gp, wg = main_call(shifted.reshape(NT, C), cotangent.reshape(NT, C), pool.reshape(2, NS, 256),
                                  w_query, w_key, w_value, w_out)
    pooled, weights = reduce_call(gp, wg)
    share = jnp.broadcast_to((pooled * (1.0 / 64.0)).reshape(6, 1, 2, 1, C), (6, 8, 2, 8, C)).reshape(48, 16, C)
    grad_features = (base.reshape(48, 16, C) + share).astype(BF16)
    grads = weights.reshape(2, 4, C, 256).transpose(1, 2, 0, 3).reshape(4, C, C).astype(F32)
    return (out.reshape(48, 16, C), grad_features, grads[0], grads[1], grads[2], grads[3])


def solution(mesh):
    tile = P("row", "col", None)
    return jax.shard_map(body, mesh=mesh, in_specs=(tile, tile, P(), P(), P(), P()),
                         out_specs=(tile, tile, P(), P(), P(), P()), check_vma=False)
```

```python
import jax, jax.numpy as jnp
from jax import lax
from jax.experimental import pallas as pl
from jax.experimental.pallas import tpu as pltpu
from jax.sharding import PartitionSpec as P

C = 512
NS = 1536
NT = 768
F32, BF16 = jnp.float32, jnp.bfloat16


def dot(a, b):
    return jnp.dot(a, b, preferred_element_type=F32)


def dot_t(a, b):
    return lax.dot_general(a, b, (((1,), (1,)), ((), ())), preferred_element_type=F32)


def main_kernel(f_ref, cot_ref, wq_ref, wk_ref, wv_ref, wo_ref,
                out_ref, base_ref, gp_ref, wg_ref,
                x_ref, pool_ref, mean, other, mine, sem_s, sem_r, kp, vp, kt, vt, qt, gt, s_scr, we, ds, att_t, gq_t, gk, gv, acc_k, acc_v):
    first_row = lax.axis_index("row") == 0
    first_col = lax.axis_index("col") == 0
    halo, finish_gather = start_gather(f_ref, x_ref, pool_ref, mean, other, mine, sem_s, sem_r)

    def put_keys(src, first, count):
        for w_ref, dst, dst_t in ((wk_ref, kp, kt), (wv_ref, vp, vt)):
            val = src(w_ref).astype(BF16)
            for p in range(4):
                dst[p, first:first + count, :] = val[:, p * 128:(p + 1) * 128]
            for i in range(count // 128):
                tr = val[i * 128:(i + 1) * 128].T
                for h in range(8):
                    dst_t[h, 0:64, first + i * 128:first + (i + 1) * 128] = tr[h * 64:(h + 1) * 64]
    for copy in halo:
        copy.wait()
    for w in range(3):
        xw = x_ref[w * 16:(w + 1) * 16].reshape(256, C)
        put_keys(lambda wr: dot(xw, wr[...]), NS + w * 256, 256)
        qt[w] = (dot(xw, wq_ref[...]).astype(BF16) * jnp.asarray(0.125, BF16)).T
        gt[w] = dot_t(wo_ref[...], cot_ref[w * 256:(w + 1) * 256]).astype(BF16)
    tail = (lax.broadcasted_iota(jnp.int32, (16, 2304), 0) == 0).astype(F32).astype(BF16)
    for h in range(8):
        vt[h, 64:80, :] = tail
    acc_k[...] = jnp.zeros_like(acc_k)
    acc_v[...] = jnp.zeros_like(acc_v)
    finish_gather()

    def pool_rows(half, i):
        return pool_ref[half, i * 16:(i + 1) * 16].reshape(384, 256)

    for i in range(4):
        put_keys(lambda w: dot(pool_rows(0, i), w[0:256]) + dot(pool_rows(1, i), w[256:512]),
                 i * 384, 384)

    def step(it, carry):
        p = it // 3
        w = it % 3
        kwin = pl.ds(pl.multiple_of(NS + w * 256, 256), 256)
        def regions(axis):
            idx = lax.broadcasted_iota(jnp.int32, (256, 256), axis)
            r = jnp.where(((idx // 16) < 8) & first_row & (w == 0), 2, 0)
            return r + jnp.where(((idx % 16) < 8) & first_col, 1, 0)
        def rows_of(ref, c):
            return ref[p, c * 256:(c + 1) * 256, :] if c < 6 else ref[p, kwin, :]
        zeros = jnp.zeros((64, 256), BF16)
        pads = (lambda v: jnp.concatenate([v, zeros], 0), lambda v: jnp.concatenate([zeros, v], 0))
        sides = []
        for hh in range(2):
            h = p * 2 + hh
            hs = pl.ds(pl.multiple_of(h * 64, 64), 64)
            q = qt[w, hs, :]
            g = gt[w, hs, :]
            qm, gm = pads[hh](q), pads[hh](g)
            m8 = None
            for c in range(7):
                s = dot(rows_of(kp, c), qm)
                if c == 6:
                    s = jnp.where(regions(0) == regions(1), s, -1e30)
                s_scr[hh, c * 256:(c + 1) * 256, :] = s
                top = jnp.max(s.reshape(32, 8, 256), axis=0)
                m8 = top if m8 is None else jnp.maximum(m8, top)
            m = jnp.max(m8, axis=0, keepdims=True)
            for c in range(7):
                we[hh, c * 256:(c + 1) * 256, :] = jnp.exp(s_scr[hh, c * 256:(c + 1) * 256, :] - m).astype(BF16)
            a80 = dot(vt[h, :, 0:NS], we[hh, 0:NS, :]) + dot(vt[h, :, kwin], we[hh, NS:, :])
            rinv = 1.0 / a80[64:65, :]
            att = a80[0:64, :] * rinv
            att_t[w, hs, :] = att.astype(BF16)
            inner = jnp.sum(att * g.astype(F32), axis=0, keepdims=True)
            for c in range(7):
                dp = dot(rows_of(vp, c), gm)
                ds[hh, c * 256:(c + 1) * 256, :] = (we[hh, c * 256:(c + 1) * 256, :].astype(F32) * (dp - inner)).astype(BF16)
            dq = dot(kt[h, :, 0:NS], ds[hh, 0:NS, :]) + dot(kt[h, :, kwin], ds[hh, NS:, :])
            gq_t[w, hs, :] = (dq * (rinv * 0.125)).astype(BF16)
            sides.append(((qm.astype(F32) * rinv).astype(BF16), (gm.astype(F32) * rinv).astype(BF16)))
        for c in range(7):
            rows = slice(c * 256, (c + 1) * 256)
            dk = dot_t(ds[0, rows, :], sides[0][0]) + dot_t(ds[1, rows, :], sides[1][0])
            dv = dot_t(we[0, rows, :], sides[0][1]) + dot_t(we[1, rows, :], sides[1][1])
            if c < 6:
                acc_k[p, rows, :] += dk
                acc_v[p, rows, :] += dv
            else:
                gk[w, p] = dk.astype(BF16)
                gv[w, p] = dv.astype(BF16)
        return carry

    lax.fori_loop(0, 12, step, 0)

    wg_acc = [None] * 4
    for w in range(3):
        rows = slice(w * 256, (w + 1) * 256)
        xw = x_ref[w * 16:(w + 1) * 16].reshape(256, C)
        cw = cot_ref[rows]
        a_t = att_t[w]
        out_ref[rows] = (xw.astype(F32) + dot(a_t.T, wo_ref[...])).astype(BF16)
        gqw = gq_t[w].T
        gkw = jnp.concatenate([gk[w, p] for p in range(4)], 1)
        gvw = jnp.concatenate([gv[w, p] for p in range(4)], 1)
        base_ref[rows] = cw.astype(F32) + dot_t(gqw, wq_ref[...]) + dot_t(gkw, wk_ref[...]) + dot_t(gvw, wv_ref[...])
        xt = xw.T
        for i, (a, b) in enumerate(((xt, gqw), (xt, gkw), (xt, gvw), (a_t, cw))):
            t = dot(a, b)
            wg_acc[i] = t if w == 0 else wg_acc[i] + t
    sk = jnp.concatenate([acc_k[p].astype(BF16) for p in range(4)], 1)
    sv = jnp.concatenate([acc_v[p].astype(BF16) for p in range(4)], 1)
    for i in range(4):
        rows = slice(i * 384, (i + 1) * 384)
        gp_ref[rows] = (dot_t(sk[rows], wk_ref[...]) + dot_t(sv[rows], wv_ref[...])).astype(BF16)
        pt = jnp.concatenate([pool_rows(0, i).T, pool_rows(1, i).T], 0)
        wg_acc[1] += dot(pt, sk[rows])
        wg_acc[2] += dot(pt, sv[rows])
    for i in range(4):
        wg_ref[i * 512:(i + 1) * 512] = wg_acc[i].astype(BF16)


def main_call(features, cot, wq, wk, wv, wo):
    vm = pl.BlockSpec(memory_space=pltpu.VMEM)
    return pl.pallas_call(
        main_kernel,
        out_shape=(jax.ShapeDtypeStruct((NT, C), BF16), jax.ShapeDtypeStruct((NT, C), F32),
                   jax.ShapeDtypeStruct((NS, C), BF16), jax.ShapeDtypeStruct((2048, C), BF16)),
        in_specs=[vm] * 6, out_specs=(vm,) * 4,
        scratch_shapes=[
            pltpu.VMEM((48, 16, C), BF16), pltpu.VMEM((2, CHIPS, 24, 256), BF16),
            pltpu.VMEM((16, C), F32), pltpu.VMEM((16, 256), F32), pltpu.VMEM((24, 256), BF16),
            pltpu.SemaphoreType.DMA((7,)), pltpu.SemaphoreType.DMA((6,)),
            pltpu.VMEM((4, 2304, 128), BF16), pltpu.VMEM((4, 2304, 128), BF16),
            pltpu.VMEM((8, 64, 2304), BF16), pltpu.VMEM((8, 80, 2304), BF16),
            pltpu.VMEM((3, 512, 256), BF16), pltpu.VMEM((3, 512, 256), BF16),
            pltpu.VMEM((2, 1792, 256), F32), pltpu.VMEM((2, 1792, 256), BF16), pltpu.VMEM((2, 1792, 256), BF16),
            pltpu.VMEM((3, 512, 256), BF16), pltpu.VMEM((3, 512, 256), BF16),
            pltpu.VMEM((3, 4, 256, 128), BF16), pltpu.VMEM((3, 4, 256, 128), BF16),
            pltpu.VMEM((4, NS, 128), F32), pltpu.VMEM((4, NS, 128), F32),
        ],
        compiler_params=pltpu.CompilerParams(vmem_limit_bytes=60 * 1024 * 1024, collective_id=0, has_side_effects=True),
        name="attention",
    )(features, cot, wq, wk, wv, wo)


ROWS, COLS, CHIPS = 8, 16, 64
MESH_ID = pl.DeviceIdType.MESH


def place():
    row, col = lax.axis_index("row"), lax.axis_index("col")
    core = lax.rem(col, 2)
    return row, col, core, row * 8 + lax.div(col, 2)


def chip_device(chip, core):
    return (lax.div(chip, 8), lax.rem(chip, 8) * 2 + core)


def neighbour(row, col, down, right):
    return (lax.rem(row + down + ROWS, ROWS), lax.rem(col + right + COLS, COLS))


def meet(row, col, core, chip):
    barrier = pltpu.get_barrier_semaphore()

    def greet(i, carry):
        pl.semaphore_signal(barrier, inc=1, device_id=chip_device(lax.rem(chip + i, CHIPS), core), device_id_type=MESH_ID)
        return carry

    lax.fori_loop(1, CHIPS, greet, 0)
    for down, right in ((0, 1), (1, 1), (0, -1), (-1, -1)):
        pl.semaphore_signal(barrier, inc=1, device_id=neighbour(row, col, down, right), device_id_type=MESH_ID)
    return barrier


def remote(src, dst, send, recv, device):
    return pltpu.make_async_remote_copy(src_ref=src, dst_ref=dst, send_sem=send, recv_sem=recv,
                                        device_id=device, device_id_type=MESH_ID)


def to_all_chips(src_of, dst, send, recv, chip, core):
    def one(i, carry):
        peer = lax.rem(chip + i, CHIPS)
        remote(src_of(peer), dst, send, recv, chip_device(peer, core)).start()
        return carry

    lax.fori_loop(1, CHIPS, one, 0)


def drain(buf, sem):
    pltpu.make_async_copy(buf, buf, sem).wait()


def start_gather(f_ref, shifted_ref, pool_ref, mean, other, mine, sem_s, sem_r):
    row, col, core, chip = place()
    partner = (row, col + 1 - 2 * core)
    barrier = meet(row, col, core, chip)
    for i in range(6):
        total = jnp.sum(f_ref[8 * i:8 * i + 8].astype(F32), axis=0)
        mean[2 * i:2 * i + 2, :] = jnp.sum(total.reshape(2, 8, C), axis=1) * (1.0 / 64.0)
    mean[12:16, :] = jnp.zeros((4, C), F32)
    pl.semaphore_wait(barrier, CHIPS - 1 + 4)
    swap = remote(mean.at[:, pl.ds(pl.multiple_of((1 - core) * 256, 256), 256)], other, sem_s.at[0], sem_r.at[0], partner)
    swap.start()
    halo = [
        remote(f_ref.at[0:40, 8:16], shifted_ref.at[8:48, 0:8], sem_s.at[1], sem_r.at[1], neighbour(row, col, 0, 1)),
        remote(f_ref.at[40:48, 0:8], shifted_ref.at[0:8, 8:16], sem_s.at[2], sem_r.at[2], neighbour(row, col, 1, 0)),
        remote(f_ref.at[40:48, 8:16], shifted_ref.at[0:8, 0:8], sem_s.at[3], sem_r.at[3], neighbour(row, col, 1, 1)),
    ]
    swap.wait()
    own = mean[:, pl.ds(pl.multiple_of(core * 256, 256), 256)]
    got = other[...]
    first = jnp.where(core == 0, own, got)
    second = jnp.where(core == 0, got, own)
    mine[...] = jnp.concatenate([first[0:12], second[0:12]], 0).astype(BF16)
    to_all_chips(lambda peer: mine, pool_ref.at[core, chip], sem_s.at[4], sem_r.at[4], chip, core)
    for copy in halo:
        copy.start()
    keep = pltpu.make_async_copy(mine, pool_ref.at[core, chip], sem_s.at[6])
    keep.start()
    shifted_ref[8:48, 8:16, :] = f_ref[0:40, 0:8, :]

    def finish():
        keep.wait()
        drain(pool_ref.at[core, 0:CHIPS - 1], sem_r.at[4])
        last = remote(pool_ref.at[core], pool_ref.at[core], sem_s.at[5], sem_r.at[5], partner)
        last.start()
        drain(pool_ref.at[core, 0:CHIPS - 1], sem_s.at[4])
        last.wait()

    return halo, finish


def reduce_kernel(gp_ref, wg_ref, pooled_ref, weights_ref,
                  gp_in, wg_in, gp_s, wg_s, gp_r, wg_r, half, half_in, block, block_in, mine, sem_s, sem_r):
    row, col, core, chip = place()
    partner = (row, col + 1 - 2 * core)
    barrier = meet(row, col, core, chip)
    pl.semaphore_wait(barrier, CHIPS - 1 + 4)
    theirs = pl.ds(pl.multiple_of((1 - core) * 256, 256), 256)
    ours = pl.ds(pl.multiple_of(core * 256, 256), 256)
    swap_w = remote(wg_ref.at[1 - core], wg_in, sem_s.at[0], sem_r.at[0], partner)
    swap_g = remote(gp_ref.at[:, :, theirs], gp_in, sem_s.at[1], sem_r.at[1], partner)
    swap_w.start()
    swap_g.start()

    def add_up(a, b, dst):
        def one(i, carry):
            dst[i] = (a(i).astype(F32) + b[i].astype(F32)).astype(BF16)
            return carry
        lax.fori_loop(0, CHIPS, one, 0)

    def total(buf, rows, lanes):
        def one(i, carry):
            return carry + buf[i].astype(F32)
        return lax.fori_loop(0, CHIPS, one, jnp.zeros((rows, lanes), F32))

    swap_w.wait()
    add_up(lambda i: wg_ref[core, i], wg_in, wg_s)
    to_all_chips(lambda peer: wg_s.at[peer], wg_r.at[chip], sem_s.at[2], sem_r.at[2], chip, core)
    swap_g.wait()
    add_up(lambda i: gp_ref[i, :, ours], gp_in, gp_s)
    to_all_chips(lambda peer: gp_s.at[peer], gp_r.at[chip], sem_s.at[3], sem_r.at[3], chip, core)
    wg_r[chip] = wg_s[chip]
    gp_r[chip] = gp_s[chip]
    drain(wg_r.at[0:CHIPS - 1], sem_r.at[2])
    mine[...] = total(wg_r, 16, C).astype(BF16)
    to_all_chips(lambda peer: mine, weights_ref.at[core, chip], sem_s.at[4], sem_r.at[4], chip, core)
    keep = pltpu.make_async_copy(mine, weights_ref.at[core, chip], sem_s.at[7])
    keep.start()
    drain(gp_r.at[0:CHIPS - 1], sem_r.at[3])
    half[...] = total(gp_r, 24, 256)
    swap_h = remote(half, half_in, sem_s.at[5], sem_r.at[5], partner)
    swap_h.start()
    swap_h.wait()
    own, got = half[...], half_in[...]
    both = jnp.concatenate([jnp.where(core == 0, own, got), jnp.where(core == 0, got, own)], 1)
    block[0:12, :] = jnp.where(core == 0, both[0:12], both[12:24])
    block[12:16, :] = jnp.zeros((4, C), F32)
    spread = [remote(block, block_in.at[k], sem_s.at[8 + k], sem_r.at[6 + k], neighbour(row, col, *way))
              for k, way in enumerate(((0, 1), (1, 0), (1, 1)))]
    for copy in spread:
        copy.start()
    for copy in spread:
        copy.wait()
    for i in range(6):
        for j in range(2):
            src = (5 if i == 0 else i - 1) * 2 + 1 - j
            if i == 0:
                val = block_in[2, src:src + 1, :] if j == 0 else block_in[1, src:src + 1, :]
            else:
                val = block_in[0, src:src + 1, :] if j == 0 else block[src:src + 1, :]
            pooled_ref[2 * i + j:2 * i + j + 1, :] = val
    keep.wait()
    drain(weights_ref.at[core, 0:CHIPS - 1], sem_r.at[4])
    last = remote(weights_ref.at[core], weights_ref.at[core], sem_s.at[6], sem_r.at[9], partner)
    last.start()
    drain(wg_r.at[0:CHIPS - 1], sem_s.at[2])
    drain(gp_r.at[0:CHIPS - 1], sem_s.at[3])
    drain(weights_ref.at[core, 0:CHIPS - 1], sem_s.at[4])
    last.wait()


def reduce_call(gp, wg):
    vm = pl.BlockSpec(memory_space=pltpu.VMEM)
    return pl.pallas_call(
        reduce_kernel,
        out_shape=(jax.ShapeDtypeStruct((12, C), F32), jax.ShapeDtypeStruct((2, CHIPS, 16, C), BF16)),
        in_specs=[vm, vm], out_specs=(vm, vm),
        scratch_shapes=[
            pltpu.VMEM((CHIPS, 24, 256), BF16), pltpu.VMEM((CHIPS, 16, C), BF16),
            pltpu.VMEM((CHIPS, 24, 256), BF16), pltpu.VMEM((CHIPS, 16, C), BF16),
            pltpu.VMEM((CHIPS, 24, 256), BF16), pltpu.VMEM((CHIPS, 16, C), BF16),
            pltpu.VMEM((24, 256), F32), pltpu.VMEM((24, 256), F32),
            pltpu.VMEM((16, C), F32), pltpu.VMEM((3, 16, C), F32), pltpu.VMEM((16, C), BF16),
            pltpu.SemaphoreType.DMA((11,)), pltpu.SemaphoreType.DMA((10,)),
        ],
        compiler_params=pltpu.CompilerParams(collective_id=1, has_side_effects=True),
        name="reduce",
    )(gp.reshape(CHIPS, 24, C), wg.reshape(2, CHIPS, 16, C))


def body(features, cotangent, w_query, w_key, w_value, w_out):
    out, base, gp, wg = main_call(features, cotangent.reshape(NT, C), w_query, w_key, w_value, w_out)
    pooled, weights = reduce_call(gp, wg)
    share = jnp.broadcast_to((pooled * (1.0 / 64.0)).reshape(6, 1, 2, 1, C), (6, 8, 2, 8, C)).reshape(48, 16, C)
    grad_features = (base.reshape(48, 16, C) + share).astype(BF16)
    grads = weights.reshape(4, C, C).astype(F32)
    return (out.reshape(48, 16, C), grad_features, grads[0], grads[1], grads[2], grads[3])


def solution(mesh):
    tile = P("row", "col", None)
    return jax.shard_map(body, mesh=mesh, in_specs=(tile, tile, P(), P(), P(), P()),
                         out_specs=(tile, tile, P(), P(), P(), P()), check_vma=False)
```
